32 devices in a mesh: parts: 2 (over x), row: 16 (over z, y, core).
Axes of the slice: x: 2, y: 2, z: 4, core: 2. Of those that a mesh axis runs over, the one named last changes fastest.
Arguments:
- sigma_top: bfloat16 [4096, 2048], P(('parts', 'row')), parts along dimension 0, may hold values from -2 to 8, as said below
- panel_par: bfloat16 [4096, 1024], P(('parts', 'row')), parts along dimension 0, may hold values from -0.25 to 0.25
- dinv_par: float32 [2048, 1024], P(('parts', 'row')), parts along dimension 0, may hold values from -2 to 8, as said below
- panel_kid_top: bfloat16 [4, 2048, 1024], P('parts', 'row'), parts along dimension 0, may hold values from -0.25 to 0.25
- panel_kid_par: bfloat16 [4, 1024, 1024], P('parts', 'row'), parts along dimension 0, may hold values from -0.375 to 0.375
- dvar_kid: float32 [4, 1024], P('parts'), parts along dimension 0, may hold values from 0.5 to 2
- mask_par: int32 [16, 4], P('parts'), parts along dimension 0, may hold values 0 or 1
- mask_kid_top: int32 [4, 8, 4], P('parts'), parts along dimension 0, may hold values 0 or 1
- mask_kid_par: int32 [4, 4, 4], P('parts'), parts along dimension 0, may hold values 0 or 1
Outputs:
- cross_par: bfloat16 [4096, 1024], P(('parts', 'row')), parts along dimension 0
- sigma_par: bfloat16 [2048, 1024], P(('parts', 'row')), parts along dimension 0
- cross_kid_top: bfloat16 [4, 2048, 1024], P('parts', 'row'), parts along dimension 0
- cross_kid_par: bfloat16 [4, 1024, 1024], P('parts', 'row'), parts along dimension 0
- variance_kid: float32 [4, 1024], P('parts'), parts along dimension 0
The draws below stay inside these ranges and needn't reach their ends.
There are 2 independent parts, one for each index of `parts`. The reference program is written for one: setup_inputs(seed, part) draws one part's arguments, and reference() takes and returns one part's arrays. A program takes and returns all parts, laid end to end along the dimension named above; each array names one. Nothing has to cross between parts.
Inputs may be any that keep to these rules, and one draw needn't show every extreme that they name: `sigma_top`: symmetric positive definite. `dinv_par`: symmetric positive definite.
All inputs are finite; a program needn't handle non-finite values.
Results may differ from the reference program's by a relative error of at most 0.0052.
Values may be sent and summed in bfloat16 or wider, within the bound.
A program may use at most 64 MiB of HBM per device.

```python
import math
import jax
import jax.numpy as jnp
from jax import lax

WT = 2048
W1 = 1024
W2 = 1024
BLK = 256
KIDS = 2


def definite(key, width):
    first, second = jax.random.split(key, 2)
    raw = jax.random.normal(first, (width, width), jnp.float32)
    sym = (raw + raw.T) * (0.25 / jnp.sqrt(jnp.float32(width)))
    diag_part = jax.random.uniform(second, (width,), jnp.float32, 1.0, 2.0)
    whole = sym + jnp.diag(diag_part)
    return whole


def draw_sigma_top(key, part):
    return definite(jax.random.fold_in(key, 11), WT).astype(jnp.bfloat16)


def draw_dinv_par(key, part):
    return definite(jax.random.fold_in(key, 23), W1)


def place_ends(entries, key, low, high):
    longest = entries.shape.index(max(entries.shape))
    spots = []
    for shift in (0, 1):
        where = [jax.random.randint(jax.random.fold_in(key, axis), (), 0, length) for axis, length in enumerate(entries.shape)]
        where[longest] = (where[longest] + shift) % entries.shape[longest]
        spots.append(tuple(where))
    return entries.at[spots[0]].set(low).at[spots[1]].set(high)


def block_scale(rng, extent, shards, smallest, high):
    def one(position, parts):
        steps = jax.random.uniform(jax.random.fold_in(jax.random.fold_in(rng, 6), position), (parts,), jnp.float32, smallest / len(shards), high / len(shards))
        return jnp.repeat(jnp.exp(steps), extent[position] // parts).reshape((-1,) + (1,) * (len(extent) - position - 1))

    level = one(*shards[0])
    for cut in shards[1:]:
        level = level * one(*cut)
    return level


def noise(own_key, shape, spread, reach, cuts=(), dtype=jnp.bfloat16):
    entries = jax.random.normal(own_key, shape, jnp.float32) * spread
    if len(cuts) > 0:
        entries = block_scale(own_key, shape, cuts, -0.22, 0.18) * entries
    return jnp.clip(entries, min=-reach, max=reach).astype(dtype)


def setup_inputs(seed: int = 0, part: int = 0) -> dict:
    arg_keys = jax.random.split(jax.random.key(seed), 10)
    part_splits = jax.random.split(jax.random.fold_in(arg_keys[9], part), 10)
    return {
        "sigma_top": draw_sigma_top(jax.random.fold_in(jax.random.fold_in(arg_keys[9], part), 71), part),
        "panel_par": noise(part_splits[1], (WT, W1), (WT // 4) ** -0.5, 0.25, ((0, 16),)),
        "dinv_par": draw_dinv_par(jax.random.fold_in(jax.random.fold_in(arg_keys[9], part), 71), part),
        "panel_kid_top": noise(part_splits[3], (KIDS, WT, W2), (WT // 4) ** -0.5, 0.25, ((1, 16),)),
        "panel_kid_par": noise(part_splits[4], (KIDS, W1, W2), (W1 // 4) ** -0.5, 0.375, ((1, 16),)),
        "dvar_kid": jnp.clip(jnp.exp(jax.random.uniform(part_splits[5], (KIDS, W2), jnp.float32, math.log(0.5), math.log(2.0))), 0.5, 2.0),
        "mask_par": place_ends((jax.random.randint(part_splits[6], (WT // BLK, W1 // BLK), 0, 3) < 2).astype(jnp.int32), jax.random.fold_in(part_splits[6], 1), 0, 1),
        "mask_kid_top": place_ends((jax.random.randint(part_splits[7], (KIDS, WT // BLK, W2 // BLK), 0, 3) < 2).astype(jnp.int32), jax.random.fold_in(part_splits[7], 1), 0, 1),
        "mask_kid_par": place_ends((jax.random.randint(part_splits[8], (KIDS, W1 // BLK, W2 // BLK), 0, 3) < 2).astype(jnp.int32), jax.random.fold_in(part_splits[8], 1), 0, 1),
    }


def widen(mask):
    grown = jnp.repeat(jnp.repeat(mask, BLK, axis=-2), BLK, axis=-1)
    return grown.astype(jnp.bfloat16)


def reference(sigma_top, panel_par, dinv_par, panel_kid_top, panel_kid_par, dvar_kid, mask_par, mask_kid_top, mask_kid_par):
    high = lax.Precision.HIGHEST
    par_masked = panel_par * widen(mask_par)
    kid_top_masked = panel_kid_top * widen(mask_kid_top)
    kid_par_masked = panel_kid_par * widen(mask_kid_par)
    cross_par = jnp.dot(sigma_top, par_masked, preferred_element_type=jnp.float32).astype(jnp.bfloat16)
    sigma_par = (dinv_par + jnp.dot(par_masked.T, cross_par, preferred_element_type=jnp.float32)).astype(jnp.bfloat16)
    sig_wide = sigma_top.astype(jnp.float32)
    cross_wide = cross_par.astype(jnp.float32)
    spar_wide = sigma_par.astype(jnp.float32)
    ktop_wide = kid_top_masked.astype(jnp.float32)
    kpar_wide = kid_par_masked.astype(jnp.float32)
    kid_top = jnp.einsum("ac,kcw->kaw", sig_wide, ktop_wide, precision=high)
    kid_top = kid_top + jnp.einsum("ap,kpw->kaw", cross_wide, kpar_wide, precision=high)
    cross_kid_top = kid_top.astype(jnp.bfloat16)
    kid_par = jnp.einsum("ap,kaw->kpw", cross_wide, ktop_wide, precision=high)
    kid_par = kid_par + jnp.einsum("pq,kqw->kpw", spar_wide, kpar_wide, precision=high)
    cross_kid_par = kid_par.astype(jnp.bfloat16)
    variance_kid = dvar_kid + jnp.sum(ktop_wide * cross_kid_top.astype(jnp.float32), axis=1)
    variance_kid = variance_kid + jnp.sum(kpar_wide * cross_kid_par.astype(jnp.float32), axis=1)
    return cross_par, sigma_par, cross_kid_top, cross_kid_par, variance_kid
```

```python
import functools

import jax
import jax.numpy as jnp
from jax import lax
from jax.experimental import pallas as pl
from jax.experimental.pallas import tpu as pltpu
from jax.sharding import PartitionSpec as P

BLK = 256
TILE = 256
MESH = pl.DeviceIdType.MESH
ACROSS_FIRST = (False, False, False, True)


def block_mask(mask, rows, first):
    index = (first + jnp.arange(rows, dtype=jnp.int32)) // BLK
    picker = (index[:, None] == jnp.arange(mask.shape[-2], dtype=jnp.int32)[None, :]).astype(
        jnp.float32
    )
    picked = jnp.einsum("rb,...bc->...rc", picker, mask.astype(jnp.float32))
    return jnp.repeat(picked, BLK, axis=-1).astype(jnp.bfloat16)


def shards(
    sigma_top,
    panel_par,
    dinv_par,
    panel_kid_top,
    panel_kid_par,
    dvar_kid,
    mask_par,
    mask_kid_top,
    mask_kid_par,
):
    rows_top = sigma_top.shape[0]
    rows_par = dinv_par.shape[0]
    position = lax.axis_index("row")
    par_masked = panel_par * block_mask(mask_par, rows_top, position * rows_top)
    kid_top_masked = panel_kid_top * block_mask(mask_kid_top, rows_top, position * rows_top)
    kid_par_masked = panel_kid_par * block_mask(mask_kid_par, rows_par, position * rows_par)
    columns = sigma_top
    cross_wide = jnp.dot(
        columns,
        lax.all_gather(par_masked, "row", axis=0, tiled=True),
        preferred_element_type=jnp.float32,
    )
    cross_par = cross_wide.astype(jnp.bfloat16)
    turned = lax.all_to_all(par_masked, "row", split_axis=1, concat_axis=0, tiled=True)
    panel_rows = turned.T
    columns = panel_rows
    diag_sum = jnp.dot(
        columns,
        lax.all_gather(cross_par, "row", axis=0, tiled=True),
        preferred_element_type=jnp.float32,
    )
    sigma_par = (dinv_par + diag_sum).astype(jnp.bfloat16)
    turned_cross = lax.all_to_all(cross_par, "row", split_axis=1, concat_axis=0, tiled=True)
    cross_rows_par = turned_cross.T
    piece = lax.all_gather(kid_top_masked, "row", axis=1, tiled=True)
    upper = jnp.einsum("rc,kcw->krw", sigma_top, piece, preferred_element_type=jnp.float32)
    lower = jnp.einsum("rc,kcw->krw", cross_rows_par, piece, preferred_element_type=jnp.float32)
    acc_top = upper
    acc_par = lower
    piece = lax.all_gather(kid_par_masked, "row", axis=1, tiled=True)
    upper = acc_top + jnp.einsum(
        "rc,kcw->krw", cross_par, piece, preferred_element_type=jnp.float32
    )
    lower = acc_par + jnp.einsum(
        "rc,kcw->krw", sigma_par, piece, preferred_element_type=jnp.float32
    )
    cross_kid_top = upper.astype(jnp.bfloat16)
    cross_kid_par = lower.astype(jnp.bfloat16)
    partial_var = jnp.sum(
        kid_top_masked.astype(jnp.float32) * cross_kid_top.astype(jnp.float32), axis=1
    )
    partial_var = partial_var + jnp.sum(
        kid_par_masked.astype(jnp.float32) * cross_kid_par.astype(jnp.float32), axis=1
    )
    variance_kid = dvar_kid + lax.psum(partial_var, "row")
    return (cross_par, sigma_par, cross_kid_top, cross_kid_par, variance_kid)


def fused(
    n, par, kt, kp, sig, dinv, dvar,
    o_cross, o_sp, o_ckt, o_ckp, o_var,
    gpar, gkt, gkp, lhs1, lhs2, acc, ct, part, slots,
    send_sem, recv_sem, turn_send, turn_recv, var_send, var_recv,
):
    me = lax.axis_index("row")
    c = me % 2
    b = (me // 2) % 2
    a = me // 4
    line = n // 4
    rows_top = par.shape[0]
    rows_par = kp.shape[1]
    wide = par.shape[1]
    tiles = wide // TILE
    RIGHT, LEFT, ACROSS, PEER = range(4)

    def at(a_, b_, c_):
        return (a_ * 2 + b_) * 2 + c_

    targets = (at(a + 1, b, c), at(a - 1, b, c), at(a, 1 - b, c), at(a, b, 1 - c))

    def own(k):
        return (par, kt.at[0], kp, kt.at[1])[k]

    def slot(k, o):
        top = pl.ds(pl.multiple_of(o * rows_top, rows_top), rows_top)
        low = pl.ds(pl.multiple_of(o * rows_par, rows_par), rows_par)
        if k == 0:
            return gpar.at[top, :]
        if k == 2:
            return gkp.at[:, low, :]
        return gkt.at[0 if k == 1 else 1, top, :]

    def copy(k, o, way, mine=False):
        return pltpu.make_async_remote_copy(
            src_ref=own(k) if mine else slot(k, o),
            dst_ref=slot(k, o),
            send_sem=send_sem.at[way, k, o],
            recv_sem=recv_sem.at[k, o],
            device_id={"row": targets[way]},
            device_id_type=MESH,
        )

    ends = []

    def send(k, o, way, mine=False, cond=None):
        limit = {RIGHT: a < line - 1, LEFT: a > 0}.get(way)
        if limit is not None:
            cond = limit if cond is None else jnp.logical_and(cond, limit)

        def go():
            copy(k, o, way, mine).start()

        def end():
            copy(k, o, way, mine).wait_send()

        if cond is None:
            go()
            ends.append(end)
        else:
            pl.when(cond)(go)
            ends.append(lambda: pl.when(cond)(end))

    def got(k, o, cond=None):
        def go():
            copy(k, o, PEER).wait_recv()

        if cond is None:
            go()
        else:
            pl.when(cond)(go)

    def start_across(k):
        send(k, me, ACROSS, True)

    def start_line(k):
        send(k, me, RIGHT, True)
        send(k, me, LEFT, True)
        if not ACROSS_FIRST[k]:
            send(k, me, ACROSS, True)
        send(k, me, PEER, True)

    def step(k, s, way, b_):
        o = at(a - s, b_, c) if way == RIGHT else at(a + s, b_, c)
        cond = a >= s if way == RIGHT else a + s < line
        got(k, o, cond)
        send(k, o, way, cond=cond)
        if not ACROSS_FIRST[k]:
            send(k, o, ACROSS, cond=cond)
        send(k, o, PEER, cond=cond)

    def crossed(k, s):
        for sign in (-1, 1) if s else (1,):
            o = at(a + sign * s, 1 - b, c)
            cond = None if s == 0 else (a >= s if sign < 0 else a + s < line)
            got(k, o, cond)
            if ACROSS_FIRST[k]:
                send(k, o, RIGHT, cond=cond)
                send(k, o, LEFT, cond=cond)
            send(k, o, PEER, cond=cond)

    def peers(k):
        for a_ in range(line):
            for b_ in range(2):
                got(k, at(a_, b_, 1 - c))

    todo = []

    def work(count=1):
        for _ in range(count):
            if todo:
                todo.pop(0)()

    def cols(t):
        return pl.ds(t * TILE, TILE)

    def cross_tile(t):
        wide_sum = jnp.dot(sig[...], gpar[:, cols(t)], preferred_element_type=jnp.float32)
        value = wide_sum.astype(jnp.bfloat16)
        o_cross[:, cols(t)] = value
        lhs2[pl.ds(0, rows_top), cols(t)] = value
        ct[cols(t), :] = wide_sum.T.astype(jnp.bfloat16)

    def turn(j):
        return pltpu.make_async_remote_copy(
            src_ref=ct.at[pl.ds(pl.multiple_of(j * rows_par, rows_par), rows_par), :],
            dst_ref=lhs1.at[
                pl.ds(rows_top, rows_par), pl.ds(pl.multiple_of(me * rows_top, rows_top), rows_top)
            ],
            send_sem=turn_send.at[j],
            recv_sem=turn_recv.at[me],
            device_id={"row": j},
            device_id_type=MESH,
        )

    def turn_start():
        for d in range(1, n):
            turn((me + d) % n).start()
        lhs1[pl.ds(rows_top, rows_par), pl.ds(pl.multiple_of(me * rows_top, rows_top), rows_top)] = ct[
            pl.ds(pl.multiple_of(me * rows_par, rows_par), rows_par), :
        ]

    def turn_end():
        for d in range(1, n):
            o = (me + d) % n
            here = lhs1.at[
                pl.ds(rows_top, rows_par), pl.ds(pl.multiple_of(o * rows_top, rows_top), rows_top)
            ]
            pltpu.make_async_remote_copy(
                src_ref=here,
                dst_ref=here,
                send_sem=turn_send.at[o],
                recv_sem=turn_recv.at[o],
                device_id={"row": o},
                device_id_type=MESH,
            ).wait_recv()

    def sigma_tile(t):
        value = dinv[:, cols(t)] + jnp.dot(
            lhs1[pl.ds(rows_top, rows_par), :], gpar[:, cols(t)], preferred_element_type=jnp.float32
        )
        value = value.astype(jnp.bfloat16)
        o_sp[:, cols(t)] = value
        lhs2[pl.ds(rows_top, rows_par), cols(t)] = value

    def low_tile(k, t):
        total = jnp.dot(lhs2[...], gkp[k, :, cols(t)], preferred_element_type=jnp.float32)
        acc[k, :, cols(t)] = total

    def top_tile(k, t):
        return jnp.dot(lhs1[...], gkt[k, :, cols(t)], preferred_element_type=jnp.float32)

    def first_top(t):
        acc[0, :, cols(t)] = top_tile(0, t)

    def finish(k, t, total):
        value = (acc[k, :, cols(t)] + total).astype(jnp.bfloat16)
        o_ckt[k, :, cols(t)] = value[:rows_top]
        o_ckp[k, :, cols(t)] = value[rows_top:]
        back = value.astype(jnp.float32)
        var = jnp.sum(kt[k, :, cols(t)].astype(jnp.float32) * back[:rows_top], axis=0, keepdims=True)
        var = var + jnp.sum(
            kp[k, :, cols(t)].astype(jnp.float32) * back[rows_top:], axis=0, keepdims=True
        )
        part[pl.ds(k, 1), cols(t)] = var

    def finish_first(t):
        finish(0, t, jnp.dot(lhs2[...], gkp[0, :, cols(t)], preferred_element_type=jnp.float32))

    barrier = pltpu.get_barrier_semaphore()
    for d in range(1, n):
        pl.semaphore_signal(
            barrier, inc=1, device_id={"row": (me + d) % n}, device_id_type=MESH
        )
    pl.semaphore_wait(barrier, n - 1)

    start_line(0)
    for k in range(4):
        if ACROSS_FIRST[k]:
            start_across(k)
    start_line(1)
    top = pl.ds(pl.multiple_of(me * rows_top, rows_top), rows_top)
    low = pl.ds(pl.multiple_of(me * rows_par, rows_par), rows_par)
    gpar[top, :] = par[...]
    gkt[:, top, :] = kt[...]
    gkp[:, low, :] = kp[...]
    lhs1[pl.ds(0, rows_top), :] = sig[...]

    late = []
    for k in range(4):
        if k + 2 < 4:
            pre = k + 2
        else:
            pre = None
        sides = (b, 1 - b) if ACROSS_FIRST[k] else (b,)
        if ACROSS_FIRST[k]:
            crossed(k, 0)
        for s in range(1, line):
            for b_ in sides:
                for way in (RIGHT, LEFT):
                    step(k, s, way, b_)
            if s == 1 and pre is not None:
                start_line(pre)
            while late:
                late.pop(0)()
            if not ACROSS_FIRST[k]:
                late.append(functools.partial(crossed, k, s - 1))
            work(4)
        if not ACROSS_FIRST[k]:
            late.append(functools.partial(crossed, k, line - 1))
        if k == 0:
            todo.append(lambda: (peers(0), cross_tile(0)))
            todo.extend(functools.partial(cross_tile, t) for t in range(1, tiles))
            todo.append(turn_start)
        if k == 1:
            todo.append(turn_end)
            todo.extend(functools.partial(sigma_tile, t) for t in range(tiles))
            todo.append(lambda: (peers(1), first_top(0)))
            todo.extend(functools.partial(first_top, t) for t in range(1, tiles))
        if k == 2:
            todo.append(lambda: (peers(2), finish_first(0)))
            todo.extend(functools.partial(finish_first, t) for t in range(1, tiles))
            todo.extend(functools.partial(low_tile, 1, t) for t in range(tiles))
    while late:
        late.pop(0)()
    work(len(todo))
    peers(3)
    for t in range(tiles):
        finish(1, t, top_tile(1, t))

    def var_copy(j, o):
        return pltpu.make_async_remote_copy(
            src_ref=part,
            dst_ref=slots.at[o],
            send_sem=var_send.at[j],
            recv_sem=var_recv.at[o],
            device_id={"row": j},
            device_id_type=MESH,
        )

    for d in range(1, n):
        var_copy((me + d) % n, me).start()
    slots[me] = part[...]
    for end in ends:
        end()
    for d in range(1, n):
        turn((me + d) % n).wait_send()
    for d in range(1, n):
        other = (me + d) % n
        var_copy(other, other).wait_recv()
    total = dvar[...]
    for o in range(n):
        total = total + slots[o]
    o_var[...] = total
    for d in range(1, n):
        var_copy((me + d) % n, me).wait_send()


def fused_shards(
    n,
    sigma_top,
    panel_par,
    dinv_par,
    panel_kid_top,
    panel_kid_par,
    dvar_kid,
    mask_par,
    mask_kid_top,
    mask_kid_par,
):
    rows_top, width_top = sigma_top.shape
    rows_par, width_par = dinv_par.shape
    kids, _, width_kid = panel_kid_top.shape
    position = lax.axis_index("row")
    par_masked = panel_par * block_mask(mask_par, rows_top, position * rows_top)
    kid_top_masked = panel_kid_top * block_mask(mask_kid_top, rows_top, position * rows_top)
    kid_par_masked = panel_kid_par * block_mask(mask_kid_par, rows_par, position * rows_par)
    bf16, f32 = jnp.bfloat16, jnp.float32
    rows = rows_top + rows_par
    sem = pltpu.SemaphoreType.DMA
    return pl.pallas_call(
        functools.partial(fused, n),
        out_shape=(
            jax.ShapeDtypeStruct((rows_top, width_par), bf16),
            jax.ShapeDtypeStruct((rows_par, width_par), bf16),
            jax.ShapeDtypeStruct((kids, rows_top, width_kid), bf16),
            jax.ShapeDtypeStruct((kids, rows_par, width_kid), bf16),
            jax.ShapeDtypeStruct((kids, width_kid), f32),
        ),
        in_specs=[pl.BlockSpec(memory_space=pltpu.VMEM)] * 6,
        out_specs=[pl.BlockSpec(memory_space=pltpu.VMEM)] * 5,
        scratch_shapes=[
            pltpu.VMEM((width_top, width_par), bf16),
            pltpu.VMEM((kids, width_top, width_kid), bf16),
            pltpu.VMEM((kids, width_par, width_kid), bf16),
            pltpu.VMEM((rows, width_top), bf16),
            pltpu.VMEM((rows, width_par), bf16),
            pltpu.VMEM((kids, rows, width_kid), f32),
            pltpu.VMEM((width_par, rows_top), bf16),
            pltpu.VMEM((kids, width_kid), f32),
            pltpu.VMEM((n, kids, width_kid), f32),
            sem((4, 4, n)),
            sem((4, n)),
            sem((n,)),
            sem((n,)),
            sem((n,)),
            sem((n,)),
        ],
        compiler_params=pltpu.CompilerParams(
            collective_id=0, has_side_effects=True, vmem_limit_bytes=56 * 2**20
        ),
        name="fused",
    )(par_masked, kid_top_masked, kid_par_masked, sigma_top, dinv_par, dvar_kid)


def choose(n, *args):
    rows_top, rows_par, kids = args[0].shape[0], args[2].shape[0], args[3].shape[0]
    fits = rows_top % 128 == 0 and rows_par % 16 == 0 and n % 4 == 0 and kids == 2
    fits = fits and args[1].shape[1] % TILE == 0 and args[1].shape[1] == args[3].shape[2]
    return fused_shards(n, *args) if fits else shards(*args)


def solution(mesh):
    return jax.shard_map(
        functools.partial(choose, mesh.shape["row"]),
        mesh=mesh,
        in_specs=(
            P(("parts", "row"), None),
            P(("parts", "row"), None),
            P(("parts", "row"), None),
            P("parts", "row", None),
            P("parts", "row", None),
            P("parts", None),
            P("parts", None),
            P("parts", None, None),
            P("parts", None, None),
        ),
        out_specs=(
            P(("parts", "row"), None),
            P(("parts", "row"), None),
            P("parts", "row", None),
            P("parts", "row", None),
            P("parts", None),
        ),
        check_vma=False,
    )
```

```python
import functools

import jax
import jax.numpy as jnp
from jax import lax
from jax.experimental import pallas as pl
from jax.experimental.pallas import tpu as pltpu
from jax.sharding import PartitionSpec as P

BLK = 256
TILE = 256
MESH = pl.DeviceIdType.MESH
ACROSS_FIRST = (False, False, False, True)
LAG = 5


def block_mask(mask, rows, first):
    index = (first + jnp.arange(rows, dtype=jnp.int32)) // BLK
    picker = (index[:, None] == jnp.arange(mask.shape[-2], dtype=jnp.int32)[None, :]).astype(
        jnp.float32
    )
    picked = jnp.einsum("rb,...bc->...rc", picker, mask.astype(jnp.float32))
    return jnp.repeat(picked, BLK, axis=-1).astype(jnp.bfloat16)


def shards(
    sigma_top,
    panel_par,
    dinv_par,
    panel_kid_top,
    panel_kid_par,
    dvar_kid,
    mask_par,
    mask_kid_top,
    mask_kid_par,
):
    rows_top = sigma_top.shape[0]
    rows_par = dinv_par.shape[0]
    position = lax.axis_index("row")
    par_masked = panel_par * block_mask(mask_par, rows_top, position * rows_top)
    kid_top_masked = panel_kid_top * block_mask(mask_kid_top, rows_top, position * rows_top)
    kid_par_masked = panel_kid_par * block_mask(mask_kid_par, rows_par, position * rows_par)
    columns = sigma_top
    cross_wide = jnp.dot(
        columns,
        lax.all_gather(par_masked, "row", axis=0, tiled=True),
        preferred_element_type=jnp.float32,
    )
    cross_par = cross_wide.astype(jnp.bfloat16)
    turned = lax.all_to_all(par_masked, "row", split_axis=1, concat_axis=0, tiled=True)
    panel_rows = turned.T
    columns = panel_rows
    diag_sum = jnp.dot(
        columns,
        lax.all_gather(cross_par, "row", axis=0, tiled=True),
        preferred_element_type=jnp.float32,
    )
    sigma_par = (dinv_par + diag_sum).astype(jnp.bfloat16)
    turned_cross = lax.all_to_all(cross_par, "row", split_axis=1, concat_axis=0, tiled=True)
    cross_rows_par = turned_cross.T
    piece = lax.all_gather(kid_top_masked, "row", axis=1, tiled=True)
    upper = jnp.einsum("rc,kcw->krw", sigma_top, piece, preferred_element_type=jnp.float32)
    lower = jnp.einsum("rc,kcw->krw", cross_rows_par, piece, preferred_element_type=jnp.float32)
    acc_top = upper
    acc_par = lower
    piece = lax.all_gather(kid_par_masked, "row", axis=1, tiled=True)
    upper = acc_top + jnp.einsum(
        "rc,kcw->krw", cross_par, piece, preferred_element_type=jnp.float32
    )
    lower = acc_par + jnp.einsum(
        "rc,kcw->krw", sigma_par, piece, preferred_element_type=jnp.float32
    )
    cross_kid_top = upper.astype(jnp.bfloat16)
    cross_kid_par = lower.astype(jnp.bfloat16)
    partial_var = jnp.sum(
        kid_top_masked.astype(jnp.float32) * cross_kid_top.astype(jnp.float32), axis=1
    )
    partial_var = partial_var + jnp.sum(
        kid_par_masked.astype(jnp.float32) * cross_kid_par.astype(jnp.float32), axis=1
    )
    variance_kid = dvar_kid + lax.psum(partial_var, "row")
    return (cross_par, sigma_par, cross_kid_top, cross_kid_par, variance_kid)


def fused(
    n, mpar, mkt, mkp, par, kt, kp, sig, dinv, dvar,
    o_cross, o_sp, o_ckt, o_ckp, o_var,
    gpar, gkt, gkp, lhs1, lhs2, acc, ct, part, slots,
    send_sem, recv_sem, turn_send, turn_recv, var_send, var_recv,
):
    me = lax.axis_index("row")
    c = me % 2
    b = (me // 2) % 2
    a = me // 4
    line = n // 4
    rows_top = par.shape[0]
    rows_par = kp.shape[1]
    wide = par.shape[1]
    tiles = wide // TILE
    RIGHT, LEFT, ACROSS, PEER = range(4)

    def at(a_, b_, c_):
        return (a_ * 2 + b_) * 2 + c_

    targets = (at(a + 1, b, c), at(a - 1, b, c), at(a, 1 - b, c), at(a, b, 1 - c))

    def own(k):
        return (par, kt.at[0], kp, kt.at[1])[k]

    def slot(k, o):
        top = pl.ds(pl.multiple_of(o * rows_top, rows_top), rows_top)
        low = pl.ds(pl.multiple_of(o * rows_par, rows_par), rows_par)
        if k == 0:
            return gpar.at[top, :]
        if k == 2:
            return gkp.at[:, low, :]
        return gkt.at[0 if k == 1 else 1, top, :]

    def copy(k, o, way, mine=False):
        return pltpu.make_async_remote_copy(
            src_ref=own(k) if mine else slot(k, o),
            dst_ref=slot(k, o),
            send_sem=send_sem.at[way, k, o],
            recv_sem=recv_sem.at[k, o],
            device_id={"row": targets[way]},
            device_id_type=MESH,
        )

    ends = []

    def send(k, o, way, mine=False, cond=None):
        limit = {RIGHT: a < line - 1, LEFT: a > 0}.get(way)
        if limit is not None:
            cond = limit if cond is None else jnp.logical_and(cond, limit)

        def go():
            copy(k, o, way, mine).start()

        def end():
            copy(k, o, way, mine).wait_send()

        if cond is None:
            go()
            ends.append(end)
        else:
            pl.when(cond)(go)
            ends.append(lambda: pl.when(cond)(end))

    def got(k, o, cond=None):
        def go():
            copy(k, o, PEER).wait_recv()

        if cond is None:
            go()
        else:
            pl.when(cond)(go)

    def start_across(k):
        send(k, me, ACROSS, True)

    def start_line(k):
        send(k, me, RIGHT, True)
        send(k, me, LEFT, True)
        if not ACROSS_FIRST[k]:
            send(k, me, ACROSS, True)
        send(k, me, PEER, True)

    def step(k, s, way, b_):
        o = at(a - s, b_, c) if way == RIGHT else at(a + s, b_, c)
        cond = a >= s if way == RIGHT else a + s < line
        got(k, o, cond)
        send(k, o, way, cond=cond)
        if not ACROSS_FIRST[k]:
            send(k, o, ACROSS, cond=cond)
        send(k, o, PEER, cond=cond)

    def crossed(k, s):
        for sign in (-1, 1) if s else (1,):
            o = at(a + sign * s, 1 - b, c)
            cond = None if s == 0 else (a >= s if sign < 0 else a + s < line)
            got(k, o, cond)
            if ACROSS_FIRST[k]:
                send(k, o, RIGHT, cond=cond)
                send(k, o, LEFT, cond=cond)
            send(k, o, PEER, cond=cond)

    def peers(k):
        for a_ in range(line):
            for b_ in range(2):
                got(k, at(a_, b_, 1 - c))

    todo = []

    def work(count=1):
        for _ in range(count):
            if todo:
                todo.pop(0)()

    def cols(t):
        return pl.ds(t * TILE, TILE)

    def masked(values, mask, first, t):
        count = values.shape[0] // BLK
        return jnp.concatenate(
            [
                values[r * BLK : (r + 1) * BLK]
                * mask[first + r, t].astype(jnp.float32).astype(jnp.bfloat16)
                for r in range(count)
            ],
            axis=0,
        )

    blocks_top = gkt.shape[1] // BLK
    blocks_par = gkp.shape[1] // BLK

    def all_par(t):
        return masked(gpar[:, cols(t)], mpar, 0, t)

    def all_kt(k, t):
        return masked(gkt[k, :, cols(t)], mkt, k * blocks_top, t)

    def all_kp(k, t):
        return masked(gkp[k, :, cols(t)], mkp, k * blocks_par, t)

    def cross_tile(t):
        wide_sum = jnp.dot(sig[...], all_par(t), preferred_element_type=jnp.float32)
        value = wide_sum.astype(jnp.bfloat16)
        o_cross[:, cols(t)] = value
        lhs2[pl.ds(0, rows_top), cols(t)] = value
        ct[cols(t), :] = wide_sum.T.astype(jnp.bfloat16)

    def turn(j):
        return pltpu.make_async_remote_copy(
            src_ref=ct.at[pl.ds(pl.multiple_of(j * rows_par, rows_par), rows_par), :],
            dst_ref=lhs1.at[
                pl.ds(rows_top, rows_par), pl.ds(pl.multiple_of(me * rows_top, rows_top), rows_top)
            ],
            send_sem=turn_send.at[j],
            recv_sem=turn_recv.at[me],
            device_id={"row": j},
            device_id_type=MESH,
        )

    def turn_start():
        for d in range(1, n):
            turn((me + d) % n).start()
        lhs1[pl.ds(rows_top, rows_par), pl.ds(pl.multiple_of(me * rows_top, rows_top), rows_top)] = ct[
            pl.ds(pl.multiple_of(me * rows_par, rows_par), rows_par), :
        ]

    def turn_end():
        for d in range(1, n):
            o = (me + d) % n
            here = lhs1.at[
                pl.ds(rows_top, rows_par), pl.ds(pl.multiple_of(o * rows_top, rows_top), rows_top)
            ]
            pltpu.make_async_remote_copy(
                src_ref=here,
                dst_ref=here,
                send_sem=turn_send.at[o],
                recv_sem=turn_recv.at[o],
                device_id={"row": o},
                device_id_type=MESH,
            ).wait_recv()

    def sigma_tile(t):
        value = dinv[:, cols(t)] + jnp.dot(
            lhs1[pl.ds(rows_top, rows_par), :], all_par(t), preferred_element_type=jnp.float32
        )
        value = value.astype(jnp.bfloat16)
        o_sp[:, cols(t)] = value
        lhs2[pl.ds(rows_top, rows_par), cols(t)] = value

    def low_tile(k, t):
        total = jnp.dot(lhs2[...], all_kp(k, t), preferred_element_type=jnp.float32)
        acc[k, :, cols(t)] = total

    def top_tile(k, t):
        return jnp.dot(lhs1[...], all_kt(k, t), preferred_element_type=jnp.float32)

    def first_top(t):
        acc[0, :, cols(t)] = top_tile(0, t)

    def finish(k, t, total):
        value = (acc[k, :, cols(t)] + total).astype(jnp.bfloat16)
        o_ckt[k, :, cols(t)] = value[:rows_top]
        o_ckp[k, :, cols(t)] = value[rows_top:]
        back = value.astype(jnp.float32)
        top_part = jnp.sum(
            kt[k, :, cols(t)].astype(jnp.float32) * back[:rows_top], axis=0, keepdims=True
        )
        low_part = jnp.sum(
            kp[k, :, cols(t)].astype(jnp.float32) * back[rows_top:], axis=0, keepdims=True
        )
        top_on = mkt[k * blocks_top + me * rows_top // BLK, t].astype(jnp.float32)
        low_on = mkp[k * blocks_par + me * rows_par // BLK, t].astype(jnp.float32)
        part[pl.ds(k, 1), cols(t)] = top_part * top_on + low_part * low_on

    def finish_first(t):
        finish(0, t, jnp.dot(lhs2[...], all_kp(0, t), preferred_element_type=jnp.float32))

    barrier = pltpu.get_barrier_semaphore()
    for d in range(1, n):
        pl.semaphore_signal(
            barrier, inc=1, device_id={"row": (me + d) % n}, device_id_type=MESH
        )
    pl.semaphore_wait(barrier, n - 1)

    start_line(0)
    for k in range(4):
        if ACROSS_FIRST[k]:
            start_across(k)
    start_line(1)
    top = pl.ds(pl.multiple_of(me * rows_top, rows_top), rows_top)
    low = pl.ds(pl.multiple_of(me * rows_par, rows_par), rows_par)
    gpar[top, :] = par[...]
    gkt[:, top, :] = kt[...]
    gkp[:, low, :] = kp[...]
    lhs1[pl.ds(0, rows_top), :] = sig[...]

    def ready(k):
        if k == 0:
            todo.append(lambda: (peers(0), cross_tile(0)))
            todo.extend(functools.partial(cross_tile, t) for t in range(1, tiles))
            todo.append(turn_start)
        if k == 1:
            todo.append(lambda: (peers(1), turn_end(), first_top(0)))
            todo.extend(functools.partial(first_top, t) for t in range(1, tiles))
            todo.extend(functools.partial(sigma_tile, t) for t in range(tiles))
        if k == 2:
            todo.append(lambda: (peers(2), finish_first(0)))
            todo.extend(functools.partial(finish_first, t) for t in range(1, tiles))
            todo.extend(functools.partial(low_tile, 1, t) for t in range(tiles))

    late = {}
    now = 0
    for k in range(4):
        sides = (b, 1 - b) if ACROSS_FIRST[k] else (b,)
        if not ACROSS_FIRST[k]:
            for s in range(line):
                late.setdefault(now + s + LAG, []).append((k, s))
        for s in range(1, line):
            now += 1
            for b_ in sides:
                for way in (RIGHT, LEFT):
                    step(k, s, way, b_)
            if s == 1 and k + 2 < 4:
                start_line(k + 2)
            if s == 1 and k + 1 < 4 and ACROSS_FIRST[k + 1]:
                crossed(k + 1, 0)
            for k_, s_ in late.pop(now, []):
                crossed(k_, s_)
                if s_ == line - 1:
                    ready(k_)
            work(4)
    for when in sorted(late):
        for k_, s_ in late[when]:
            crossed(k_, s_)
            if s_ == line - 1:
                ready(k_)
    work(len(todo))
    peers(3)
    for t in range(tiles):
        finish(1, t, top_tile(1, t))

    def var_copy(j, o):
        return pltpu.make_async_remote_copy(
            src_ref=part,
            dst_ref=slots.at[o],
            send_sem=var_send.at[j],
            recv_sem=var_recv.at[o],
            device_id={"row": j},
            device_id_type=MESH,
        )

    for d in range(1, n):
        var_copy((me + d) % n, me).start()
    slots[me] = part[...]
    for end in ends:
        end()
    for d in range(1, n):
        turn((me + d) % n).wait_send()
    for d in range(1, n):
        other = (me + d) % n
        var_copy(other, other).wait_recv()
    total = dvar[...]
    for o in range(n):
        total = total + slots[o]
    o_var[...] = total
    for d in range(1, n):
        var_copy((me + d) % n, me).wait_send()


def fused_shards(
    n,
    sigma_top,
    panel_par,
    dinv_par,
    panel_kid_top,
    panel_kid_par,
    dvar_kid,
    mask_par,
    mask_kid_top,
    mask_kid_par,
):
    rows_top, width_top = sigma_top.shape
    rows_par, width_par = dinv_par.shape
    kids, _, width_kid = panel_kid_top.shape
    bf16, f32 = jnp.bfloat16, jnp.float32
    rows = rows_top + rows_par
    sem = pltpu.SemaphoreType.DMA
    return pl.pallas_call(
        functools.partial(fused, n),
        out_shape=(
            jax.ShapeDtypeStruct((rows_top, width_par), bf16),
            jax.ShapeDtypeStruct((rows_par, width_par), bf16),
            jax.ShapeDtypeStruct((kids, rows_top, width_kid), bf16),
            jax.ShapeDtypeStruct((kids, rows_par, width_kid), bf16),
            jax.ShapeDtypeStruct((kids, width_kid), f32),
        ),
        in_specs=[pl.BlockSpec(memory_space=pltpu.SMEM)] * 3
        + [pl.BlockSpec(memory_space=pltpu.VMEM)] * 6,
        out_specs=[pl.BlockSpec(memory_space=pltpu.VMEM)] * 5,
        scratch_shapes=[
            pltpu.VMEM((width_top, width_par), bf16),
            pltpu.VMEM((kids, width_top, width_kid), bf16),
            pltpu.VMEM((kids, width_par, width_kid), bf16),
            pltpu.VMEM((rows, width_top), bf16),
            pltpu.VMEM((rows, width_par), bf16),
            pltpu.VMEM((kids, rows, width_kid), f32),
            pltpu.VMEM((width_par, rows_top), bf16),
            pltpu.VMEM((kids, width_kid), f32),
            pltpu.VMEM((n, kids, width_kid), f32),
            sem((4, 4, n)),
            sem((4, n)),
            sem((n,)),
            sem((n,)),
            sem((n,)),
            sem((n,)),
        ],
        compiler_params=pltpu.CompilerParams(
            collective_id=0, has_side_effects=True, vmem_limit_bytes=56 * 2**20
        ),
        name="fused",
    )(
        mask_par,
        mask_kid_top.reshape(-1, mask_kid_top.shape[-1]),
        mask_kid_par.reshape(-1, mask_kid_par.shape[-1]),
        panel_par,
        panel_kid_top,
        panel_kid_par,
        sigma_top,
        dinv_par,
        dvar_kid,
    )


def choose(n, *args):
    rows_top, rows_par, kids = args[0].shape[0], args[2].shape[0], args[3].shape[0]
    fits = rows_top % 128 == 0 and rows_par % 16 == 0 and n % 4 == 0 and kids == 2
    fits = fits and BLK % rows_top == 0 and BLK % rows_par == 0 and TILE == BLK
    fits = fits and args[1].shape[1] % TILE == 0 and args[1].shape[1] == args[3].shape[2]
    return fused_shards(n, *args) if fits else shards(*args)


def solution(mesh):
    return jax.shard_map(
        functools.partial(choose, mesh.shape["row"]),
        mesh=mesh,
        in_specs=(
            P(("parts", "row"), None),
            P(("parts", "row"), None),
            P(("parts", "row"), None),
            P("parts", "row", None),
            P("parts", "row", None),
            P("parts", None),
            P("parts", None),
            P("parts", None, None),
            P("parts", None, None),
        ),
        out_specs=(
            P(("parts", "row"), None),
            P(("parts", "row"), None),
            P("parts", "row", None),
            P("parts", "row", None),
            P("parts", None),
        ),
        check_vma=False,
    )
```
